32 devices in a mesh: dp: 4 (over x, y), ep: 8 (over z, core).
Axes of the slice: x: 2, y: 2, z: 4, core: 2. Of those that a mesh axis runs over, the one named last changes fastest.
Arguments:
- tokens: bfloat16 [8192, 2048], P(('dp', 'ep')), parts along dimension 0
- expert_ids: int32 [8192, 6], P(('dp', 'ep')), parts along dimension 0
- gate_vals: float32 [8192, 6], P(('dp', 'ep')), parts along dimension 0
- w_gate: bfloat16 [64, 2048, 1408], P('ep')
- w_up: bfloat16 [64, 2048, 1408], P('ep')
- w_down: bfloat16 [64, 1408, 2048], P('ep')
Outputs:
- output: bfloat16 [8192, 2048], P(('dp', 'ep')), parts along dimension 0
There are 4 independent parts. The reference program is written for one: setup_inputs(seed, part) draws one part's arguments, and reference() takes and returns one part's arrays. A program takes and returns all parts, laid end to end along the dimension named above; an argument that names none is the same for every part.
All inputs are finite; a program needn't handle non-finite values.
Results may differ from the reference program's by a relative error of at most 0.00665691.
Values are sent between devices in bfloat16 or wider.
A program may use at most 1 GiB of HBM per device.

```python
import jax
import jax.numpy as jnp
from jax import lax

D_MODEL = 2048
FFN_DIM = 1408
NUM_EXPERTS = 64
TOP_K = 6
GROUP = 8
TOK_DEV = 256

DEV_LIMIT = TOP_K // 2
LOCAL_EXPERTS = NUM_EXPERTS // GROUP
PAIR_CAP = TOK_DEV * DEV_LIMIT // GROUP
EXPERT_CAP = TOK_DEV * TOP_K * GROUP // NUM_EXPERTS
TOKENS = GROUP * TOK_DEV


def perm_rows(rand_key, row_count, perm_size):
    return jax.vmap(lambda sub_key: jax.random.permutation(sub_key, perm_size))(jax.random.split(rand_key, row_count))


def draw_routing(rand_key):
    key_src, key_dst, key_slot = jax.random.split(rand_key, 3)
    src_perm = perm_rows(key_src, GROUP, GROUP)
    dst_perm = perm_rows(key_dst, GROUP, LOCAL_EXPERTS)
    flat_pos = jnp.arange(TOK_DEV)[:, None] * DEV_LIMIT + jnp.arange(DEV_LIMIT)[None, :]
    dest_dev = src_perm[:, flat_pos % GROUP]
    recv_row = jnp.arange(GROUP)[:, None, None] * PAIR_CAP + (flat_pos // GROUP)[None, :, :]
    first_loc = dst_perm[dest_dev, (2 * recv_row) % LOCAL_EXPERTS]
    second_loc = dst_perm[dest_dev, (2 * recv_row + 1) % LOCAL_EXPERTS]
    pair_ids = jnp.stack([first_loc, second_loc], axis=-1) + dest_dev[..., None] * LOCAL_EXPERTS
    ordered = pair_ids.reshape(TOKENS, TOP_K)
    scores = jax.random.randint(key_slot, (TOKENS, TOP_K), 0, 1 << 20) * TOP_K + jnp.arange(TOP_K)[None, :]
    slot_order = jnp.argsort(scores, axis=1)
    return jnp.take_along_axis(ordered, slot_order, axis=1).astype(jnp.int32)


def setup_inputs(seed: int = 0, part: int = 0) -> dict:
    base_key = jax.random.key(seed)
    key_x, key_route, key_gate = jax.random.split(jax.random.fold_in(base_key, part), 3)
    key_wg, key_wu, key_wd = jax.random.split(jax.random.key(seed + 1), 3)
    in_scale = D_MODEL ** -0.5
    out_scale = 2.0 * FFN_DIM ** -0.5
    tokens = jax.random.normal(key_x, (TOKENS, D_MODEL), jnp.float32).astype(jnp.bfloat16)
    expert_ids = draw_routing(key_route)
    logits = 1.5 * jax.random.normal(key_gate, (TOKENS, TOP_K), jnp.float32)
    gate_vals = jax.nn.softmax(logits, axis=-1)
    w_gate = (in_scale * jax.random.normal(key_wg, (NUM_EXPERTS, D_MODEL, FFN_DIM), jnp.float32)).astype(jnp.bfloat16)
    w_up = (in_scale * jax.random.normal(key_wu, (NUM_EXPERTS, D_MODEL, FFN_DIM), jnp.float32)).astype(jnp.bfloat16)
    w_down = (out_scale * jax.random.normal(key_wd, (NUM_EXPERTS, FFN_DIM, D_MODEL), jnp.float32)).astype(jnp.bfloat16)
    return {'tokens': tokens, 'expert_ids': expert_ids, 'gate_vals': gate_vals, 'w_gate': w_gate, 'w_up': w_up, 'w_down': w_down}


def expert_ffn(row_in, gate_mat, up_mat, down_mat):
    gate_act = jnp.dot(row_in, gate_mat, preferred_element_type=jnp.float32)
    up_act = jnp.dot(row_in, up_mat, preferred_element_type=jnp.float32)
    hidden = (jax.nn.silu(gate_act) * up_act).astype(jnp.bfloat16)
    return jnp.dot(hidden, down_mat, preferred_element_type=jnp.float32).astype(jnp.bfloat16)


def reference(tokens, expert_ids, gate_vals, w_gate, w_up, w_down):
    pair_count = TOKENS * TOP_K
    flat_ids = expert_ids.reshape(pair_count)
    pair_index = jnp.arange(pair_count, dtype=jnp.int32)

    def one_expert(map_item):
        expert, gate_mat, up_mat, down_mat = map_item
        member = flat_ids == expert
        slot_pos = jnp.where(member, jnp.cumsum(member.astype(jnp.int32)) - 1, EXPERT_CAP)
        pair_list = jnp.full((EXPERT_CAP,), pair_count, jnp.int32).at[slot_pos].set(pair_index, mode='drop')
        row_in = tokens[jnp.minimum(pair_list, pair_count - 1) // TOP_K]
        return pair_list, expert_ffn(row_in, gate_mat, up_mat, down_mat)

    pair_lists, expert_rows = lax.map(one_expert, (jnp.arange(NUM_EXPERTS, dtype=jnp.int32), w_gate, w_up, w_down))
    pair_out = jnp.zeros((pair_count, D_MODEL), jnp.bfloat16).at[pair_lists.reshape(-1)].set(expert_rows.reshape(-1, D_MODEL), mode='drop')
    earlier = jnp.arange(TOP_K)[None, :] < jnp.arange(TOP_K)[:, None]

    def combine_block(blk_item):
        rows_in, ids_in, gate_in, outs_in = blk_item
        dev_of = ids_in // LOCAL_EXPERTS
        same_dev = dev_of[:, :, None] == dev_of[:, None, :]
        weights = jnp.where(same_dev, gate_in[:, None, :], 0.0)
        dev_sum = jnp.einsum('tjk,tkd->tjd', weights, outs_in.astype(jnp.float32)).astype(jnp.bfloat16)
        leader = jnp.logical_not(jnp.any(same_dev & earlier[None, :, :], axis=2))
        moe_sum = jnp.sum(jnp.where(leader[:, :, None], dev_sum.astype(jnp.float32), 0.0), axis=1)
        return (rows_in.astype(jnp.float32) + moe_sum).astype(jnp.bfloat16)

    output = lax.map(combine_block, (tokens.reshape(GROUP, TOK_DEV, D_MODEL), expert_ids.reshape(GROUP, TOK_DEV, TOP_K), gate_vals.reshape(GROUP, TOK_DEV, TOP_K), pair_out.reshape(GROUP, TOK_DEV, TOP_K, D_MODEL)))
    return output.reshape(TOKENS, D_MODEL)
```

```python
import functools

import jax
import jax.numpy as jnp
from jax import lax
from jax.experimental import pallas as pl
from jax.experimental.pallas import tpu as pltpu
from jax.sharding import PartitionSpec as P

MESH = pl.DeviceIdType.MESH
F32, BF16 = jnp.float32, jnp.bfloat16
WC = 256
WO = 256
DEPTH = 4
DEPTH2 = 6
FAR = 255.0


def flip(me, d):
    z, c = me // 2, me % 2
    hi, lo = z // 2, z % 2
    if d & 4:
        hi = 1 - hi
    if d & 2:
        lo = 1 - lo
    if d & 1:
        c = 1 - c
    return hi * 4 + lo * 2 + c


def dot(a, b):
    return jnp.dot(a, b, preferred_element_type=F32)


def dot_tn(a, b):
    return lax.dot_general(a, b, (((0,), (0,)), ((), ())), preferred_element_type=F32)


def dot_nt(a, b):
    return lax.dot_general(a, b, (((1,), (1,)), ((), ())), preferred_element_type=F32)


def iota(shape, dim):
    return lax.broadcasted_iota(jnp.int32, shape, dim)


def split3(g):
    hi = g.astype(BF16).astype(F32)
    rest = g - hi
    mid = rest.astype(BF16).astype(F32)
    return jnp.concatenate([hi, mid, rest - mid], axis=0).astype(BF16)


def kernel(tok, ids, gate, wg_hbm, wu_hbm, wd_hbm, out,
           near, raw, rly, xb, ret, accg, accu, hid, fan, fan_t, gb, ssum, pk, pt, pos, rpos, gsend, gtab,
           wg, wu, wd,
           raw_s, raw_r, near_s, rly_s, x_r, tab_s, tab_r, pos_s, pos_r, out_s, ret_r, w_s, wd_s):
    n_exp = accg.shape[0]
    cap = accg.shape[1]
    t_dev = tok.shape[0]
    n_ch, rows, _ = xb.shape
    n_out = ret.shape[0]
    pair = rows // 8
    top_k = ids.shape[0]

    me = lax.axis_index("ep")
    core = me % 2
    side = me // 4
    lo = (me // 2) % 2
    is_mid = (lo + side) == 1
    relay_dev = (2 - side) * 2 + core
    far = 1 - side
    far_src = ((3 * far) * 2 + core, (1 + far) * 2 + core)
    my_rank = jnp.where(is_mid, 1, 0)
    peers = [flip(me, d) for d in range(8)]

    def remote(src, dst, s, r, dev):
        return pltpu.make_async_remote_copy(
            src_ref=src, dst_ref=dst, send_sem=s, recv_sem=r, device_id={"ep": dev}, device_id_type=MESH)

    def raw_copy(ch, j, dev):
        cols = pl.ds(pl.multiple_of(ch * WC, WC), WC)
        return remote(tok.at[:, cols], raw.at[j, ch], raw_s.at[ch], raw_r.at[j, ch], dev)

    def near_copy(ch, d):
        return remote(near.at[d - 1, ch], xb.at[ch, pl.ds(me * pair, pair)],
                      near_s.at[ch, d - 1], x_r.at[ch, me], peers[d])

    def rly_copy(ch, j, d):
        return remote(rly.at[j, d - 1, ch], xb.at[ch, pl.ds(far_src[j] * pair, pair)],
                      rly_s.at[ch, j, d - 1], x_r.at[ch, far_src[j]], peers[d])

    def x_wait(ch, src):
        remote(xb.at[ch, pl.ds(src * pair, pair)], xb.at[ch, pl.ds(src * pair, pair)],
               near_s.at[ch, 0], x_r.at[ch, src], peers[1]).wait_recv()

    def w_copies(i):
        ch, e, slot = i // n_exp, i % n_exp, i % DEPTH
        rws = pl.ds(pl.multiple_of(ch * WC, WC), WC)
        return (pltpu.make_async_copy(wg_hbm.at[e, rws], wg.at[slot], w_s.at[0, slot]),
                pltpu.make_async_copy(wu_hbm.at[e, rws], wu.at[slot], w_s.at[1, slot]))

    def wd_copy(i):
        ch, e, slot = i // n_exp, i % n_exp, i % DEPTH2
        cols = pl.ds(pl.multiple_of(ch * WO, WO), WO)
        return pltpu.make_async_copy(wd_hbm.at[e, :, cols], wd.at[slot], wd_s.at[slot])

    barrier = pltpu.get_barrier_semaphore()
    for d in range(1, 8):
        pl.semaphore_signal(barrier, inc=1, device_id={"ep": peers[d]}, device_id_type=MESH)
    for i in range(DEPTH):
        for c in w_copies(i):
            c.start()
    for i in range(DEPTH2):
        wd_copy(i).start()
    pl.semaphore_wait(barrier, 7)

    raw_copy(0, my_rank, relay_dev).start()

    dev_iota = iota((8, t_dev), 0)
    chosen = jnp.zeros((8, t_dev), F32)
    for j in range(top_k):
        chosen = jnp.where(ids[j:j + 1, :] // n_exp == dev_iota, 1.0, chosen)
    tri = (iota((t_dev, t_dev), 0) <= iota((t_dev, t_dev), 1)).astype(F32).astype(BF16)
    rank = dot(chosen.astype(BF16), tri) - 1.0
    where = jnp.where(chosen > 0.0, rank, FAR)
    pos[...] = where
    pos_copy = remote(pos, rpos.at[my_rank], pos_s, pos_r.at[my_rank], relay_dev)
    pos_copy.start()
    slot_rows = iota((pair, t_dev), 0).astype(F32)
    for q in range(8):
        mat = (slot_rows == where[q:q + 1, :]).astype(F32).astype(BF16)
        pk[q] = mat
        dense = jnp.zeros((n_exp, t_dev), F32)
        for j in range(top_k):
            dense = jnp.where(ids[j:j + 1, :] == q * n_exp + dev_iota, gate[j:j + 1, :], dense)
        parts = dot_nt(split3(dense), mat)
        packed = (parts[n_exp:2 * n_exp] + parts[2 * n_exp:]) + parts[:n_exp]
        gsend[q, :, 0:pair] = packed

    def tab_copy(d):
        return remote(gsend.at[peers[d]], gtab.at[me], tab_s.at[d - 1], tab_r.at[me], peers[d])

    def tab_wait(d):
        remote(gsend.at[peers[d]], gtab.at[peers[d]], tab_s.at[d - 1], tab_r.at[peers[d]], peers[d]).wait_recv()

    for d in range(1, 8):
        tab_copy(d).start()
    gtab[me] = gsend[me]

    def near_step(ch, _):
        cols = pl.ds(pl.multiple_of(ch * WC, WC), WC)
        block = tok[:, cols]
        for d in range(1, 4):
            near[d - 1, ch] = dot(pk[peers[d]], block).astype(BF16)
        xb[ch, pl.ds(me * pair, pair)] = dot(pk[me], block).astype(BF16)

        @pl.when(ch > 0)
        def _():
            raw_copy(ch, my_rank, relay_dev).start()

        for d in (3, 2, 1):
            near_copy(ch, d).start()
        return 0

    lax.fori_loop(0, n_ch, near_step, 0)

    lane = iota((8, rows), 1)
    base = iota((8, rows), 0) * pair
    blocks = ((lane >= base) & (lane < base + pair)).astype(F32).astype(BF16)
    spread = dot_tn(where.astype(BF16), blocks)
    lane_t = iota((t_dev, rows), 1)
    lane_s = lane_t
    for q in range(1, 8):
        lane_s = lane_s - jnp.where(lane_t >= q * pair, pair, 0)
    pt[...] = (spread == lane_s.astype(F32)).astype(F32).astype(BF16)

    def zero(e, _):
        accg[e] = jnp.zeros(accg.shape[1:], F32)
        accu[e] = jnp.zeros(accu.shape[1:], F32)
        return 0

    lax.fori_loop(0, n_exp, zero, 0)

    for d in range(1, 8):
        tab_wait(d)
    gates = jnp.concatenate([gtab[p][:, :pair] for p in range(8)], axis=1)
    member = gates != 0.0
    tri_r = (iota((rows, rows), 0) <= iota((rows, rows), 1)).astype(F32).astype(BF16)
    count = dot(member.astype(F32).astype(BF16), tri_r) - 1.0
    place = jnp.where(member, count, FAR)
    place_b = place.astype(BF16)
    gate_parts = split3(gates)
    cap_rows = iota((cap, rows), 0).astype(F32)
    cap_lanes = iota((rows, cap), 1).astype(F32)
    for e in range(n_exp):
        fan[e] = (cap_rows == place[e:e + 1, :]).astype(F32).astype(BF16)
        pick = (iota((8, cap), 0) == e).astype(F32).astype(BF16)
        fan_t[e] = (dot_tn(place_b, pick) == cap_lanes).astype(F32).astype(BF16)
        pick3 = (lax.rem(iota((24, 128), 0), 8) == e).astype(F32).astype(BF16)
        gb[e] = dot_tn(gate_parts, pick3)

    def pos_wait(j):
        remote(pos, rpos.at[j], pos_s, pos_r.at[j], relay_dev).wait_recv()

    @pl.when(is_mid)
    def _():
        for j in range(2):
            pos_wait(j)

    def relay(ch):
        for j in range(2):
            raw_copy(ch, j, relay_dev).wait_recv()
            block = raw[j, ch]

            def packed(q):
                mat = (slot_rows == rpos[j, pl.ds(q, 1), :]).astype(F32).astype(BF16)
                return dot(mat, block).astype(BF16)

            for d in (3, 2, 1):
                rly[j, d - 1, ch] = packed(peers[d])
                rly_copy(ch, j, d).start()
            xb[ch, pl.ds(far_src[j] * pair, pair)] = packed(me)

    def step_in(ch, _):
        @pl.when(is_mid)
        def _():
            relay(ch)

        for d in range(1, 4):
            x_wait(ch, peers[d])

        @pl.when(is_mid)
        def _():
            for d in (5, 7):
                pass
            x_wait(ch, far_src[0] + 1 - 2 * core)
            x_wait(ch, far_src[1] + 1 - 2 * core)

        @pl.when(jnp.logical_not(is_mid))
        def _():
            for d in range(4, 8):
                x_wait(ch, peers[d])

        def expert(e, _):
            i = ch * n_exp + e
            slot = i % DEPTH
            for c in w_copies(i):
                c.wait()
            xg = dot(fan[e], xb[ch]).astype(BF16)
            accg[e] += dot(xg, wg[slot])
            accu[e] += dot(xg, wu[slot])

            @pl.when(i + DEPTH < n_ch * n_exp)
            def _():
                for c in w_copies(i + DEPTH):
                    c.start()
            return 0

        return lax.fori_loop(0, n_exp, expert, 0)

    lax.fori_loop(0, n_ch, step_in, 0)

    def act(e, _):
        g = accg[e]
        hid[e] = (g / (1.0 + jnp.exp(-g)) * accu[e]).astype(BF16)
        return 0

    lax.fori_loop(0, n_exp, act, 0)

    def ret_copy(ch, d):
        return remote(xb.at[ch, pl.ds(peers[d] * pair, pair)], ret.at[ch, pl.ds(me * pair, pair)],
                      out_s.at[ch, d - 1], ret_r.at[ch, me], peers[d])

    def ret_wait(ch, d):
        src = peers[d]
        remote(xb.at[ch, pl.ds(src * pair, pair)], ret.at[ch, pl.ds(src * pair, pair)],
               out_s.at[ch, d - 1], ret_r.at[ch, src], src).wait_recv()

    def step_out(ch, _):
        def expert(e, _):
            i = ch * n_exp + e
            slot = i % DEPTH2
            wd_copy(i).wait()
            y = dot(hid[e], wd[slot]).astype(BF16)
            z = dot(fan_t[e], y)
            g = gb[e]
            add = jnp.concatenate([g * z[:, k * 128:(k + 1) * 128] for k in range(WO // 128)], axis=1)

            @pl.when(e == 0)
            def _():
                ssum[...] = add

            @pl.when(e > 0)
            def _():
                ssum[...] += add

            @pl.when(i + DEPTH2 < n_out * n_exp)
            def _():
                wd_copy(i + DEPTH2).start()
            return 0

        lax.fori_loop(0, n_exp, expert, 0)
        xb[ch] = ssum[...].astype(BF16)
        ret[ch, pl.ds(me * pair, pair)] = ssum[pl.ds(me * pair, pair)].astype(BF16)
        for d in (7, 6, 5, 4, 3, 2, 1):
            ret_copy(ch, d).start()
        return 0

    def drain(ch, _):
        raw_copy(ch, my_rank, relay_dev).wait_send()
        for d in range(1, 4):
            near_copy(ch, d).wait_send()

        @pl.when(is_mid)
        def _():
            for j in range(2):
                for d in range(1, 4):
                    rly_copy(ch, j, d).wait_send()
        return 0

    lax.fori_loop(0, n_out, step_out, 0)
    lax.fori_loop(0, n_ch, drain, 0)
    pos_copy.wait_send()
    for d in range(1, 8):
        tab_copy(d).wait_send()

    def step_end(ch, _):
        for d in range(1, 8):
            ret_wait(ch, d)
        cols = pl.ds(pl.multiple_of(ch * WO, WO), WO)
        out[:, cols] = (tok[:, cols].astype(F32) + dot(pt[...], ret[ch])).astype(BF16)
        return 0

    lax.fori_loop(0, n_out, step_end, 0)

    def drain_out(ch, _):
        for d in range(1, 8):
            ret_copy(ch, d).wait_send()
        return 0

    lax.fori_loop(0, n_out, drain_out, 0)


def solution(mesh):
    groups = mesh.shape['ep']
    row_spec = P(('dp', 'ep'))
    expert_spec = P('ep')

    def device_step(tokens, expert_ids, gate_vals, w_gate, w_up, w_down):
        t_dev, top_k = expert_ids.shape
        d_model = tokens.shape[1]
        n_exp, _, ffn = w_gate.shape
        pair = t_dev * (top_k // 2) // groups
        cap = t_dev * top_k // n_exp
        rows = groups * pair
        n_ch, n_out = d_model // WC, d_model // WO
        vmem = pl.BlockSpec(memory_space=pltpu.VMEM)
        hbm = pl.BlockSpec(memory_space=pl.ANY)
        dma = pltpu.SemaphoreType.DMA
        return pl.pallas_call(
            kernel,
            out_shape=jax.ShapeDtypeStruct((t_dev, d_model), BF16),
            in_specs=[vmem, vmem, vmem, hbm, hbm, hbm],
            out_specs=vmem,
            scratch_shapes=[
                pltpu.VMEM((3, n_ch, pair, WC), BF16),
                pltpu.VMEM((2, n_ch, t_dev, WC), BF16),
                pltpu.VMEM((2, 3, n_ch, pair, WC), BF16),
                pltpu.VMEM((n_ch, rows, WC), BF16),
                pltpu.VMEM((n_out, rows, WO), BF16),
                pltpu.VMEM((n_exp, cap, ffn), F32),
                pltpu.VMEM((n_exp, cap, ffn), F32),
                pltpu.VMEM((n_exp, cap, ffn), BF16),
                pltpu.VMEM((n_exp, cap, rows), BF16),
                pltpu.VMEM((n_exp, rows, cap), BF16),
                pltpu.VMEM((n_exp, rows, 128), F32),
                pltpu.VMEM((rows, WO), F32),
                pltpu.VMEM((groups, pair, t_dev), BF16),
                pltpu.VMEM((t_dev, rows), BF16),
                pltpu.VMEM((8, t_dev), F32),
                pltpu.VMEM((2, 8, t_dev), F32),
                pltpu.VMEM((groups, n_exp, 128), F32),
                pltpu.VMEM((groups, n_exp, 128), F32),
                pltpu.VMEM((DEPTH, WC, ffn), BF16),
                pltpu.VMEM((DEPTH, WC, ffn), BF16),
                pltpu.VMEM((DEPTH2, ffn, WO), BF16),
                dma((n_ch,)), dma((2, n_ch)), dma((n_ch, 3)), dma((n_ch, 2, 3)), dma((n_ch, groups)),
                dma((7,)), dma((groups,)), dma, dma((2,)),
                dma((n_out, 7)), dma((n_out, groups)), dma((2, DEPTH)), dma((DEPTH2,)),
            ],
            compiler_params=pltpu.CompilerParams(
                collective_id=0, has_side_effects=True, vmem_limit_bytes=67043328),
        )(tokens, expert_ids.T, gate_vals.T, w_gate, w_up, w_down)

    return jax.shard_map(device_step, mesh=mesh, in_specs=(row_spec, row_spec, row_spec, expert_spec, expert_spec, expert_spec), out_specs=row_spec, check_vma=False)
```

```python
import functools

import jax
import jax.numpy as jnp
from jax import lax
from jax.experimental import pallas as pl
from jax.experimental.pallas import tpu as pltpu
from jax.sharding import PartitionSpec as P

MESH = pl.DeviceIdType.MESH
F32, BF16 = jnp.float32, jnp.bfloat16
WC = 256
WO = 256
DEPTH = 8
DEPTH2 = 8
RELAYED = 6
AHEAD = 3
UNROLL = 2
UNROLL2 = 4
FAR = 255.0


def flip(me, d):
    z, c = me // 2, me % 2
    hi, lo = z // 2, z % 2
    if d & 4:
        hi = 1 - hi
    if d & 2:
        lo = 1 - lo
    if d & 1:
        c = 1 - c
    return hi * 4 + lo * 2 + c


def dot(a, b):
    return jnp.dot(a, b, preferred_element_type=F32)


def dot_tn(a, b):
    return lax.dot_general(a, b, (((0,), (0,)), ((), ())), preferred_element_type=F32)


def dot_nt(a, b):
    return lax.dot_general(a, b, (((1,), (1,)), ((), ())), preferred_element_type=F32)


def iota(shape, dim):
    return lax.broadcasted_iota(jnp.int32, shape, dim)


def split3(g):
    hi = g.astype(BF16).astype(F32)
    rest = g - hi
    mid = rest.astype(BF16).astype(F32)
    return jnp.concatenate([hi, mid, rest - mid], axis=0).astype(BF16)


def kernel(tok, ids, gate, wg_hbm, wu_hbm, wd_hbm, out,
           near, direct, raw, rly, xb, ret, acc, hid, xg, fan, fan_t, gb, ssum, pk, pt, pos, rpos, gsend, gtab,
           wgu, wd,
           raw_s, raw_r, near_s, far_s, rly_s, x_r, tab_s, tab_r, pos_s, pos_r, out_s, ret_r, w_s, wd_s):
    n_exp, cap, ffn = hid.shape
    t_dev = tok.shape[0]
    n_ch, rows, _ = xb.shape
    n_out = ret.shape[0]
    pair = rows // 8
    top_k = ids.shape[0]

    me = lax.axis_index("ep")
    core = me % 2
    side = me // 4
    lo = (me // 2) % 2
    is_mid = (lo + side) == 1
    relay_dev = (2 - side) * 2 + core
    far = 1 - side
    far_src = ((3 * far) * 2 + core, (1 + far) * 2 + core)
    my_rank = jnp.where(is_mid, 1, 0)
    peers = [flip(me, d) for d in range(8)]

    def remote(src, dst, s, r, dev):
        return pltpu.make_async_remote_copy(
            src_ref=src, dst_ref=dst, send_sem=s, recv_sem=r, device_id={"ep": dev}, device_id_type=MESH)

    def raw_copy(ch, j, dev):
        cols = pl.ds(pl.multiple_of(ch * WC, WC), WC)
        return remote(tok.at[:, cols], raw.at[j, ch], raw_s.at[ch], raw_r.at[j, ch], dev)

    def near_copy(ch, d):
        return remote(near.at[d - 1, ch], xb.at[ch, pl.ds(me * pair, pair)],
                      near_s.at[ch, d - 1], x_r.at[ch, me], peers[d])

    def far_copy(ch, d):
        return remote(direct.at[d - 4, ch - RELAYED], xb.at[ch, pl.ds(me * pair, pair)],
                      far_s.at[ch - RELAYED, d - 4], x_r.at[ch, me], peers[d])

    def rly_copy(ch, j, d):
        return remote(rly.at[j, d - 1, ch], xb.at[ch, pl.ds(far_src[j] * pair, pair)],
                      rly_s.at[ch, j, d - 1], x_r.at[ch, far_src[j]], peers[d])

    def x_wait(ch, src):
        remote(xb.at[ch, pl.ds(src * pair, pair)], xb.at[ch, pl.ds(src * pair, pair)],
               near_s.at[ch, 0], x_r.at[ch, src], peers[1]).wait_recv()

    def w_copies(i):
        ch, e, slot = i // n_exp, i % n_exp, i % DEPTH
        rws = pl.ds(pl.multiple_of(ch * WC, WC), WC)
        return (pltpu.make_async_copy(wg_hbm.at[e, rws], wgu.at[slot, :, pl.ds(0, ffn)], w_s.at[0, slot]),
                pltpu.make_async_copy(wu_hbm.at[e, rws], wgu.at[slot, :, pl.ds(ffn, ffn)], w_s.at[1, slot]))

    def wd_copy(i):
        ch, e, slot = i // n_exp, i % n_exp, i % DEPTH2
        cols = pl.ds(pl.multiple_of(ch * WO, WO), WO)
        return pltpu.make_async_copy(wd_hbm.at[e, :, cols], wd.at[slot], wd_s.at[slot])

    barrier = pltpu.get_barrier_semaphore()
    for d in range(1, 8):
        pl.semaphore_signal(barrier, inc=1, device_id={"ep": peers[d]}, device_id_type=MESH)
    for i in range(DEPTH):
        for c in w_copies(i):
            c.start()

    dev_iota = iota((8, t_dev), 0)
    chosen = jnp.zeros((8, t_dev), F32)
    for j in range(top_k):
        chosen = jnp.where(ids[j:j + 1, :] // n_exp == dev_iota, 1.0, chosen)
    tri = (iota((t_dev, t_dev), 0) <= iota((t_dev, t_dev), 1)).astype(F32).astype(BF16)
    rank = dot(chosen.astype(BF16), tri) - 1.0
    where = jnp.where(chosen > 0.0, rank, FAR)
    pos[...] = where
    pos_copy = remote(pos, rpos.at[my_rank], pos_s, pos_r.at[my_rank], relay_dev)
    slot_rows = iota((pair, t_dev), 0).astype(F32)
    for q in range(8):
        mat = (slot_rows == where[q:q + 1, :]).astype(F32).astype(BF16)
        pk[q] = mat
        dense = jnp.zeros((n_exp, t_dev), F32)
        for j in range(top_k):
            dense = jnp.where(ids[j:j + 1, :] == q * n_exp + dev_iota, gate[j:j + 1, :], dense)
        parts = dot_nt(split3(dense), mat)
        packed = (parts[n_exp:2 * n_exp] + parts[2 * n_exp:]) + parts[:n_exp]
        gsend[q, :, 0:pair] = packed

    def tab_copy(d):
        return remote(gsend.at[peers[d]], gtab.at[me], tab_s.at[d - 1], tab_r.at[me], peers[d])

    def tab_wait(d):
        remote(gsend.at[peers[d]], gtab.at[peers[d]], tab_s.at[d - 1], tab_r.at[peers[d]], peers[d]).wait_recv()

    pl.semaphore_wait(barrier, 7)
    pos_copy.start()
    for d in (7, 6, 5, 4, 3, 2, 1):
        tab_copy(d).start()
    gtab[me] = gsend[me]

    def near_send(ch):
        for d in (3, 2, 1):
            near_copy(ch, d).start()

    def near_step(ch, _):
        cols = pl.ds(pl.multiple_of(ch * WC, WC), WC)
        block = tok[:, cols]

        @pl.when(ch < RELAYED)
        def _():
            raw_copy(ch, my_rank, relay_dev).start()

        @pl.when(ch >= RELAYED)
        def _():
            for d in (7, 6, 5, 4):
                direct[d - 4, ch - RELAYED] = dot(pk[peers[d]], block).astype(BF16)
                far_copy(ch, d).start()

        for d in range(1, 4):
            near[d - 1, ch] = dot(pk[peers[d]], block).astype(BF16)
        xb[ch, pl.ds(me * pair, pair)] = dot(pk[me], block).astype(BF16)

        @pl.when(jnp.logical_not(is_mid) | (ch < AHEAD))
        def _():
            near_send(ch)
        return 0

    lax.fori_loop(0, n_ch, near_step, 0)

    for d in range(1, 8):
        tab_wait(d)
    gates = jnp.concatenate([gtab[p][:, :pair] for p in range(8)], axis=1)
    member = gates != 0.0
    tri_r = (iota((rows, rows), 0) <= iota((rows, rows), 1)).astype(F32).astype(BF16)
    count = dot(member.astype(F32).astype(BF16), tri_r) - 1.0
    place = jnp.where(member, count, FAR)
    cap_rows = iota((cap, rows), 0).astype(F32)
    for e in range(n_exp):
        fan[e] = (cap_rows == place[e:e + 1, :]).astype(F32).astype(BF16)

    def pos_wait(j):
        remote(pos, rpos.at[j], pos_s, pos_r.at[j], relay_dev).wait_recv()

    @pl.when(is_mid)
    def _():
        for j in range(2):
            pos_wait(j)

    def relay(ch):
        for j in range(2):
            raw_copy(ch, j, relay_dev).wait_recv()
            block = raw[j, ch]

            def packed(q):
                mat = (slot_rows == rpos[j, pl.ds(q, 1), :]).astype(F32).astype(BF16)
                return dot(mat, block).astype(BF16)

            for d in (3, 2, 1):
                rly[j, d - 1, ch] = packed(peers[d])
                rly_copy(ch, j, d).start()
            xb[ch, pl.ds(far_src[j] * pair, pair)] = packed(me)

        @pl.when(ch + AHEAD < n_ch)
        def _():
            near_send(ch + AHEAD)

    def group(ch, first, last):
        @pl.when(is_mid & (ch < RELAYED))
        def _():
            relay(ch)

        for d in range(1, 4):
            x_wait(ch, peers[d])

        straight = jnp.logical_not(is_mid) | (ch >= RELAYED)

        @pl.when(jnp.logical_not(straight))
        def _():
            for src in far_src:
                x_wait(ch, src + 1 - 2 * core)

        @pl.when(straight)
        def _():
            for d in range(4, 8):
                x_wait(ch, peers[d])

        block = xb[ch]
        for e in range(n_exp):
            xg[e] = dot(fan[e], block).astype(BF16)

        def experts(it, _):
            for u in range(UNROLL):
                for c in w_copies(ch * n_exp + it * UNROLL + u):
                    c.wait()
            for u in range(UNROLL):
                e = it * UNROLL + u
                slot = (ch * n_exp + e) % DEPTH
                both = dot(xg[e], wgu[slot])
                if not first:
                    both = acc[e] + both
                if last:
                    g = both[:, :ffn]
                    hid[e] = (g / (1.0 + jnp.exp(-g)) * both[:, ffn:]).astype(BF16)
                else:
                    acc[e] = both
            if not last:
                for u in range(UNROLL):
                    i = ch * n_exp + it * UNROLL + u + DEPTH

                    @pl.when(i < n_ch * n_exp)
                    def _():
                        for c in w_copies(i):
                            c.start()
            return 0

        lax.fori_loop(0, n_exp // UNROLL, experts, 0)

    def middle_group(ch, _):
        group(ch, False, False)
        return 0

    def return_tables():
        lane = iota((8, rows), 1)
        base = iota((8, rows), 0) * pair
        blocks = ((lane >= base) & (lane < base + pair)).astype(F32).astype(BF16)
        spread = dot_tn(where.astype(BF16), blocks)
        lane_t = iota((t_dev, rows), 1)
        lane_s = lane_t
        for q in range(1, 8):
            lane_s = lane_s - jnp.where(lane_t >= q * pair, pair, 0)
        pt[...] = (spread == lane_s.astype(F32)).astype(F32).astype(BF16)

        place_b = place.astype(BF16)
        gate_parts = split3(gates)
        cap_lanes = iota((rows, cap), 1).astype(F32)
        for e in range(n_exp):
            pick = (iota((8, cap), 0) == e).astype(F32).astype(BF16)
            fan_t[e] = (dot_tn(place_b, pick) == cap_lanes).astype(F32).astype(BF16)
            pick3 = (lax.rem(iota((24, 128), 0), 8) == e).astype(F32).astype(BF16)
            gb[e] = dot_tn(gate_parts, pick3)

    group(0, True, False)
    for i in range(DEPTH2):
        wd_copy(i).start()
    return_tables()
    lax.fori_loop(1, n_ch - 1, middle_group, 0)
    group(n_ch - 1, False, True)

    def ret_copy(ch, d):
        return remote(xb.at[ch, pl.ds(peers[d] * pair, pair)], ret.at[ch, pl.ds(me * pair, pair)],
                      out_s.at[ch, d - 1], ret_r.at[ch, me], peers[d])

    def ret_wait(ch, d):
        src = peers[d]
        remote(xb.at[ch, pl.ds(src * pair, pair)], ret.at[ch, pl.ds(src * pair, pair)],
               out_s.at[ch, d - 1], ret_r.at[ch, src], src).wait_recv()

    def step_out(ch, _):
        def experts(it, _):
            first = ch * n_exp + it * UNROLL2
            for u in range(UNROLL2):
                wd_copy(first + u).wait()
            ys = [dot(hid[it * UNROLL2 + u], wd[(first + u) % DEPTH2]).astype(BF16) for u in range(UNROLL2)]
            add = None
            for u in range(UNROLL2):
                e = it * UNROLL2 + u
                z = dot(fan_t[e], ys[u])
                g = gb[e]
                part = jnp.concatenate([g * z[:, k * 128:(k + 1) * 128] for k in range(WO // 128)], axis=1)
                add = part if add is None else add + part

            @pl.when(it == 0)
            def _():
                ssum[...] = add

            @pl.when(it > 0)
            def _():
                ssum[...] += add

            for u in range(UNROLL2):
                @pl.when(first + u + DEPTH2 < n_out * n_exp)
                def _():
                    wd_copy(first + u + DEPTH2).start()
            return 0

        lax.fori_loop(0, n_exp // UNROLL2, experts, 0)
        xb[ch] = ssum[...].astype(BF16)
        ret[ch, pl.ds(me * pair, pair)] = ssum[pl.ds(me * pair, pair)].astype(BF16)
        for d in (7, 6, 5, 4, 3, 2, 1):
            ret_copy(ch, d).start()
        return 0

    def drain(ch, _):
        for d in range(1, 4):
            near_copy(ch, d).wait_send()

        @pl.when(ch < RELAYED)
        def _():
            raw_copy(ch, my_rank, relay_dev).wait_send()

        @pl.when(ch >= RELAYED)
        def _():
            for d in range(4, 8):
                far_copy(ch, d).wait_send()

        @pl.when(is_mid & (ch < RELAYED))
        def _():
            for j in range(2):
                for d in range(1, 4):
                    rly_copy(ch, j, d).wait_send()
        return 0

    lax.fori_loop(0, n_out, step_out, 0)
    lax.fori_loop(0, n_ch, drain, 0)
    pos_copy.wait_send()
    for d in range(1, 8):
        tab_copy(d).wait_send()

    def step_end(ch, _):
        for d in range(1, 8):
            ret_wait(ch, d)
        cols = pl.ds(pl.multiple_of(ch * WO, WO), WO)
        out[:, cols] = (tok[:, cols].astype(F32) + dot(pt[...], ret[ch])).astype(BF16)
        return 0

    lax.fori_loop(0, n_out, step_end, 0)

    def drain_out(ch, _):
        for d in range(1, 8):
            ret_copy(ch, d).wait_send()
        return 0

    lax.fori_loop(0, n_out, drain_out, 0)


def solution(mesh):
    groups = mesh.shape['ep']
    row_spec = P(('dp', 'ep'))
    expert_spec = P('ep')

    def device_step(tokens, expert_ids, gate_vals, w_gate, w_up, w_down):
        t_dev, top_k = expert_ids.shape
        d_model = tokens.shape[1]
        n_exp, _, ffn = w_gate.shape
        pair = t_dev * (top_k // 2) // groups
        cap = t_dev * top_k // n_exp
        rows = groups * pair
        n_ch, n_out = d_model // WC, d_model // WO
        vmem = pl.BlockSpec(memory_space=pltpu.VMEM)
        hbm = pl.BlockSpec(memory_space=pl.ANY)
        dma = pltpu.SemaphoreType.DMA
        return pl.pallas_call(
            kernel,
            out_shape=jax.ShapeDtypeStruct((t_dev, d_model), BF16),
            in_specs=[vmem, vmem, vmem, hbm, hbm, hbm],
            out_specs=vmem,
            scratch_shapes=[
                pltpu.VMEM((3, n_ch, pair, WC), BF16),
                pltpu.VMEM((4, max(n_ch - RELAYED, 1), pair, WC), BF16),
                pltpu.VMEM((2, RELAYED, t_dev, WC), BF16),
                pltpu.VMEM((2, 3, RELAYED, pair, WC), BF16),
                pltpu.VMEM((n_ch, rows, WC), BF16),
                pltpu.VMEM((n_out, rows, WO), BF16),
                pltpu.VMEM((n_exp, cap, 2 * ffn), F32),
                pltpu.VMEM((n_exp, cap, ffn), BF16),
                pltpu.VMEM((n_exp, cap, WC), BF16),
                pltpu.VMEM((n_exp, cap, rows), BF16),
                pltpu.VMEM((n_exp, rows, cap), BF16),
                pltpu.VMEM((n_exp, rows, 128), F32),
                pltpu.VMEM((rows, WO), F32),
                pltpu.VMEM((groups, pair, t_dev), BF16),
                pltpu.VMEM((t_dev, rows), BF16),
                pltpu.VMEM((8, t_dev), F32),
                pltpu.VMEM((2, 8, t_dev), F32),
                pltpu.VMEM((groups, n_exp, 128), F32),
                pltpu.VMEM((groups, n_exp, 128), F32),
                pltpu.VMEM((DEPTH, WC, 2 * ffn), BF16),
                pltpu.VMEM((DEPTH2, ffn, WO), BF16),
                dma((n_ch,)), dma((2, n_ch)), dma((n_ch, 3)), dma((max(n_ch - RELAYED, 1), 4)), dma((n_ch, 2, 3)), dma((n_ch, groups)),
                dma((7,)), dma((groups,)), dma, dma((2,)),
                dma((n_out, 7)), dma((n_out, groups)), dma((2, DEPTH)), dma((DEPTH2,)),
            ],
            compiler_params=pltpu.CompilerParams(
                collective_id=0, has_side_effects=True, vmem_limit_bytes=67043328),
        )(tokens, expert_ids.T, gate_vals.T, w_gate, w_up, w_down)

    return jax.shard_map(device_step, mesh=mesh, in_specs=(row_spec, row_spec, row_spec, expert_spec, expert_spec, expert_spec), out_specs=row_spec, check_vma=False)
```

```python
import functools

import jax
import jax.numpy as jnp
from jax import lax
from jax.experimental import pallas as pl
from jax.experimental.pallas import tpu as pltpu
from jax.sharding import PartitionSpec as P

MESH = pl.DeviceIdType.MESH
F32, BF16 = jnp.float32, jnp.bfloat16
WC = 256
WO = 256
DEPTH = 8
DEPTH2 = 8
RELAYED = 5
AHEAD = 3
UNROLL = 4
UNROLL2 = 4
FAR = 255.0


def flip(me, d):
    z, c = me // 2, me % 2
    hi, lo = z // 2, z % 2
    if d & 4:
        hi = 1 - hi
    if d & 2:
        lo = 1 - lo
    if d & 1:
        c = 1 - c
    return hi * 4 + lo * 2 + c


def dot(a, b):
    return jnp.dot(a, b, preferred_element_type=F32)


def dot_tn(a, b):
    return lax.dot_general(a, b, (((0,), (0,)), ((), ())), preferred_element_type=F32)


def dot_nt(a, b):
    return lax.dot_general(a, b, (((1,), (1,)), ((), ())), preferred_element_type=F32)


def iota(shape, dim):
    return lax.broadcasted_iota(jnp.int32, shape, dim)


def split3(g):
    hi = g.astype(BF16).astype(F32)
    rest = g - hi
    mid = rest.astype(BF16).astype(F32)
    return jnp.concatenate([hi, mid, rest - mid], axis=0).astype(BF16)


def kernel(tok_hbm, ids_hbm, gate_hbm, wg_hbm, wu_hbm, wd_hbm, out_hbm,
           tok, ids, gate, out, near, direct, raw, rly, xb, ret, acc, hid, xg, fan, fan_t, gb, ssum, pk, pt, pos, rpos, gsend, gtab,
           wgu, wd,
           raw_s, raw_r, near_s, far_s, rly_s, x_r, tab_s, tab_r, pos_s, pos_r, out_s, ret_r, w_s, wd_s, in_s, done_s):
    n_exp, cap, ffn = hid.shape
    t_dev = tok.shape[0]
    n_ch, rows, _ = xb.shape
    n_out = ret.shape[0]
    pair = rows // 8
    top_k = ids.shape[0]

    me = lax.axis_index("ep")
    core = me % 2
    side = me // 4
    lo = (me // 2) % 2
    is_mid = (lo + side) == 1
    relay_dev = (2 - side) * 2 + core
    far = 1 - side
    far_src = ((3 * far) * 2 + core, (1 + far) * 2 + core)
    my_rank = jnp.where(is_mid, 1, 0)
    peers = [flip(me, d) for d in range(8)]

    def remote(src, dst, s, r, dev):
        return pltpu.make_async_remote_copy(
            src_ref=src, dst_ref=dst, send_sem=s, recv_sem=r, device_id={"ep": dev}, device_id_type=MESH)

    def raw_copy(ch, j, dev):
        cols = pl.ds(pl.multiple_of(ch * WC, WC), WC)
        return remote(tok.at[:, cols], raw.at[j, ch], raw_s.at[ch], raw_r.at[j, ch], dev)

    def near_copy(ch, d):
        return remote(near.at[d - 1, ch], xb.at[ch, pl.ds(me * pair, pair)],
                      near_s.at[ch, d - 1], x_r.at[ch, me], peers[d])

    def far_copy(ch, d):
        return remote(direct.at[d - 4, ch - RELAYED], xb.at[ch, pl.ds(me * pair, pair)],
                      far_s.at[ch - RELAYED, d - 4], x_r.at[ch, me], peers[d])

    def rly_copy(ch, j, d):
        return remote(rly.at[j, d - 1, ch], xb.at[ch, pl.ds(far_src[j] * pair, pair)],
                      rly_s.at[ch, j, d - 1], x_r.at[ch, far_src[j]], peers[d])

    def x_wait(ch, src):
        remote(xb.at[ch, pl.ds(src * pair, pair)], xb.at[ch, pl.ds(src * pair, pair)],
               near_s.at[ch, 0], x_r.at[ch, src], peers[1]).wait_recv()

    def w_copies(i):
        ch, e, slot = i // n_exp, i % n_exp, i % DEPTH
        rws = pl.ds(pl.multiple_of(ch * WC, WC), WC)
        return (pltpu.make_async_copy(wg_hbm.at[e, rws], wgu.at[slot, :, pl.ds(0, ffn)], w_s.at[0, slot]),
                pltpu.make_async_copy(wu_hbm.at[e, rws], wgu.at[slot, :, pl.ds(ffn, ffn)], w_s.at[1, slot]))

    def wd_copy(i):
        ch, e, slot = i // n_exp, i % n_exp, i % DEPTH2
        cols = pl.ds(pl.multiple_of(ch * WO, WO), WO)
        return pltpu.make_async_copy(wd_hbm.at[e, :, cols], wd.at[slot], wd_s.at[slot])

    loads = [pltpu.make_async_copy(a, b, in_s.at[k]) for k, (a, b) in enumerate(
        ((ids_hbm, ids), (gate_hbm, gate), (tok_hbm, tok)))]
    for c in loads:
        c.start()
    barrier = pltpu.get_barrier_semaphore()
    for d in range(1, 8):
        pl.semaphore_signal(barrier, inc=1, device_id={"ep": peers[d]}, device_id_type=MESH)
    for i in range(DEPTH):
        for c in w_copies(i):
            c.start()

    loads[0].wait()
    loads[1].wait()
    dev_iota = iota((8, t_dev), 0)
    chosen = jnp.zeros((8, t_dev), F32)
    for j in range(top_k):
        chosen = jnp.where(ids[j:j + 1, :] // n_exp == dev_iota, 1.0, chosen)
    tri = (iota((t_dev, t_dev), 0) <= iota((t_dev, t_dev), 1)).astype(F32).astype(BF16)
    rank = dot(chosen.astype(BF16), tri) - 1.0
    where = jnp.where(chosen > 0.0, rank, FAR)
    pos[...] = where
    pos_copy = remote(pos, rpos.at[my_rank], pos_s, pos_r.at[my_rank], relay_dev)
    slot_rows = iota((pair, t_dev), 0).astype(F32)
    for q in range(8):
        mat = (slot_rows == where[q:q + 1, :]).astype(F32).astype(BF16)
        pk[q] = mat
        dense = jnp.zeros((n_exp, t_dev), F32)
        for j in range(top_k):
            dense = jnp.where(ids[j:j + 1, :] == q * n_exp + dev_iota, gate[j:j + 1, :], dense)
        parts = dot_nt(split3(dense), mat)
        packed = (parts[n_exp:2 * n_exp] + parts[2 * n_exp:]) + parts[:n_exp]
        gsend[q, :, 0:pair] = packed

    def tab_copy(d):
        return remote(gsend.at[peers[d]], gtab.at[me], tab_s.at[d - 1], tab_r.at[me], peers[d])

    def tab_wait(d):
        remote(gsend.at[peers[d]], gtab.at[peers[d]], tab_s.at[d - 1], tab_r.at[peers[d]], peers[d]).wait_recv()

    loads[2].wait()
    pl.semaphore_wait(barrier, 7)
    pos_copy.start()
    for d in (7, 6, 5, 4, 3, 2, 1):
        tab_copy(d).start()
    gtab[me] = gsend[me]

    def near_send(ch):
        for d in (3, 2, 1):
            near_copy(ch, d).start()

    def far_send(ch, from_mid, from_end):
        @pl.when(is_mid)
        def _():
            for d in from_mid:
                far_copy(ch, d).start()

        @pl.when(jnp.logical_not(is_mid))
        def _():
            for d in from_end:
                far_copy(ch, d).start()

    def near_step(ch, _):
        cols = pl.ds(pl.multiple_of(ch * WC, WC), WC)
        block = tok[:, cols]

        @pl.when(ch < RELAYED)
        def _():
            raw_copy(ch, my_rank, relay_dev).start()

        @pl.when(ch >= RELAYED)
        def _():
            for d in (7, 6, 5, 4):
                direct[d - 4, ch - RELAYED] = dot(pk[peers[d]], block).astype(BF16)
            far_send(ch, (7, 6), (5, 4))

        for d in range(1, 4):
            near[d - 1, ch] = dot(pk[peers[d]], block).astype(BF16)
        xb[ch, pl.ds(me * pair, pair)] = dot(pk[me], block).astype(BF16)

        @pl.when(jnp.logical_not(is_mid) | (ch < AHEAD))
        def _():
            near_send(ch)
        return 0

    lax.fori_loop(0, n_ch, near_step, 0)
    for ch in range(RELAYED, n_ch):
        far_send(ch, (5, 4), (7, 6))

    for d in range(1, 8):
        tab_wait(d)
    gates = jnp.concatenate([gtab[p][:, :pair] for p in range(8)], axis=1)
    member = gates != 0.0
    tri_r = (iota((rows, rows), 0) <= iota((rows, rows), 1)).astype(F32).astype(BF16)
    count = dot(member.astype(F32).astype(BF16), tri_r) - 1.0
    place = jnp.where(member, count, FAR)
    cap_rows = iota((cap, rows), 0).astype(F32)
    for e in range(n_exp):
        fan[e] = (cap_rows == place[e:e + 1, :]).astype(F32).astype(BF16)

    def pos_wait(j):
        remote(pos, rpos.at[j], pos_s, pos_r.at[j], relay_dev).wait_recv()

    @pl.when(is_mid)
    def _():
        for j in range(2):
            pos_wait(j)

    def relay(ch):
        for j in range(2):
            raw_copy(ch, j, relay_dev).wait_recv()
            block = raw[j, ch]

            def packed(q):
                mat = (slot_rows == rpos[j, pl.ds(q, 1), :]).astype(F32).astype(BF16)
                return dot(mat, block).astype(BF16)

            for d in (3, 2, 1):
                rly[j, d - 1, ch] = packed(peers[d])
                rly_copy(ch, j, d).start()
            xb[ch, pl.ds(far_src[j] * pair, pair)] = packed(me)

        @pl.when(ch + AHEAD < n_ch)
        def _():
            near_send(ch + AHEAD)

    def group(ch, first, last):
        @pl.when(is_mid & (ch < RELAYED))
        def _():
            relay(ch)

        for d in range(1, 4):
            x_wait(ch, peers[d])

        straight = jnp.logical_not(is_mid) | (ch >= RELAYED)

        @pl.when(jnp.logical_not(straight))
        def _():
            for src in far_src:
                x_wait(ch, src + 1 - 2 * core)

        @pl.when(straight)
        def _():
            for d in range(4, 8):
                x_wait(ch, peers[d])

        block = xb[ch]
        for e in range(n_exp):
            xg[e] = dot(fan[e], block).astype(BF16)

        def experts(it, _):
            for u in range(UNROLL):
                for c in w_copies(ch * n_exp + it * UNROLL + u):
                    c.wait()
            for u in range(UNROLL):
                e = it * UNROLL + u
                slot = (ch * n_exp + e) % DEPTH
                both = dot(xg[e], wgu[slot])
                if not first:
                    both = acc[e] + both
                if last:
                    g = both[:, :ffn]
                    hid[e] = (g / (1.0 + jnp.exp(-g)) * both[:, ffn:]).astype(BF16)
                else:
                    acc[e] = both
                    i = ch * n_exp + it * UNROLL + u + DEPTH

                    @pl.when(i < n_ch * n_exp)
                    def _():
                        for c in w_copies(i):
                            c.start()
            return 0

        lax.fori_loop(0, n_exp // UNROLL, experts, 0)

    def middle_group(ch, _):
        group(ch, False, False)
        return 0

    def return_tables():
        lane = iota((8, rows), 1)
        base = iota((8, rows), 0) * pair
        blocks = ((lane >= base) & (lane < base + pair)).astype(F32).astype(BF16)
        spread = dot_tn(where.astype(BF16), blocks)
        lane_t = iota((t_dev, rows), 1)
        lane_s = lane_t
        for q in range(1, 8):
            lane_s = lane_s - jnp.where(lane_t >= q * pair, pair, 0)
        pt[...] = (spread == lane_s.astype(F32)).astype(F32).astype(BF16)

        place_b = place.astype(BF16)
        gate_parts = split3(gates)
        cap_lanes = iota((rows, cap), 1).astype(F32)
        for e in range(n_exp):
            pick = (iota((8, cap), 0) == e).astype(F32).astype(BF16)
            fan_t[e] = (dot_tn(place_b, pick) == cap_lanes).astype(F32).astype(BF16)
            pick3 = (lax.rem(iota((24, 128), 0), 8) == e).astype(F32).astype(BF16)
            gb[e] = dot_tn(gate_parts, pick3)

    group(0, True, False)
    for i in range(DEPTH2):
        wd_copy(i).start()
    return_tables()
    lax.fori_loop(1, n_ch - 1, middle_group, 0)
    group(n_ch - 1, False, True)

    def ret_copy(ch, d):
        return remote(xb.at[ch, pl.ds(peers[d] * pair, pair)], ret.at[ch, pl.ds(me * pair, pair)],
                      out_s.at[ch, d - 1], ret_r.at[ch, me], peers[d])

    def ret_wait(ch, d):
        src = peers[d]
        remote(xb.at[ch, pl.ds(src * pair, pair)], ret.at[ch, pl.ds(src * pair, pair)],
               out_s.at[ch, d - 1], ret_r.at[ch, src], src).wait_recv()

    def step_out(ch, _):
        def experts(it, _):
            first = ch * n_exp + it * UNROLL2
            for u in range(UNROLL2):
                wd_copy(first + u).wait()
            ys = [dot(hid[it * UNROLL2 + u], wd[(first + u) % DEPTH2]).astype(BF16) for u in range(UNROLL2)]
            add = None
            for u in range(UNROLL2):
                e = it * UNROLL2 + u
                z = dot(fan_t[e], ys[u])
                g = gb[e]
                part = jnp.concatenate([g * z[:, k * 128:(k + 1) * 128] for k in range(WO // 128)], axis=1)
                add = part if add is None else add + part

            @pl.when(it == 0)
            def _():
                ssum[...] = add

            @pl.when(it > 0)
            def _():
                ssum[...] += add

            for u in range(UNROLL2):
                @pl.when(first + u + DEPTH2 < n_out * n_exp)
                def _():
                    wd_copy(first + u + DEPTH2).start()
            return 0

        lax.fori_loop(0, n_exp // UNROLL2, experts, 0)
        xb[ch] = ssum[...].astype(BF16)
        ret[ch, pl.ds(me * pair, pair)] = ssum[pl.ds(me * pair, pair)].astype(BF16)
        for d in (7, 6, 5, 4, 3, 2, 1):
            ret_copy(ch, d).start()
        return 0

    def drain(ch, _):
        for d in range(1, 4):
            near_copy(ch, d).wait_send()

        @pl.when(ch < RELAYED)
        def _():
            raw_copy(ch, my_rank, relay_dev).wait_send()

        @pl.when(ch >= RELAYED)
        def _():
            for d in range(4, 8):
                far_copy(ch, d).wait_send()

        @pl.when(is_mid & (ch < RELAYED))
        def _():
            for j in range(2):
                for d in range(1, 4):
                    rly_copy(ch, j, d).wait_send()
        return 0

    lax.fori_loop(0, n_out, step_out, 0)
    lax.fori_loop(0, n_ch, drain, 0)
    pos_copy.wait_send()
    for d in range(1, 8):
        tab_copy(d).wait_send()

    def done_copy(ch):
        cols = pl.ds(pl.multiple_of(ch * WO, WO), WO)
        return pltpu.make_async_copy(out.at[ch], out_hbm.at[:, cols], done_s.at[ch])

    def step_end(ch, _):
        for d in range(1, 8):
            ret_wait(ch, d)
        cols = pl.ds(pl.multiple_of(ch * WO, WO), WO)
        out[ch] = (tok[:, cols].astype(F32) + dot(pt[...], ret[ch])).astype(BF16)
        done_copy(ch).start()
        return 0

    lax.fori_loop(0, n_out, step_end, 0)

    def drain_out(ch, _):
        for d in range(1, 8):
            ret_copy(ch, d).wait_send()
        done_copy(ch).wait()
        return 0

    lax.fori_loop(0, n_out, drain_out, 0)


def solution(mesh):
    groups = mesh.shape['ep']
    row_spec = P(('dp', 'ep'))
    expert_spec = P('ep')

    def device_step(tokens, expert_ids, gate_vals, w_gate, w_up, w_down):
        t_dev, top_k = expert_ids.shape
        d_model = tokens.shape[1]
        n_exp, _, ffn = w_gate.shape
        pair = t_dev * (top_k // 2) // groups
        cap = t_dev * top_k // n_exp
        rows = groups * pair
        n_ch, n_out = d_model // WC, d_model // WO
        hbm = pl.BlockSpec(memory_space=pl.ANY)
        dma = pltpu.SemaphoreType.DMA
        return pl.pallas_call(
            kernel,
            out_shape=jax.ShapeDtypeStruct((t_dev, d_model), BF16),
            in_specs=[hbm] * 6,
            out_specs=hbm,
            scratch_shapes=[
                pltpu.VMEM((t_dev, d_model), BF16),
                pltpu.VMEM((top_k, t_dev), jnp.int32),
                pltpu.VMEM((top_k, t_dev), F32),
                pltpu.VMEM((n_out, t_dev, WO), BF16),
                pltpu.VMEM((3, n_ch, pair, WC), BF16),
                pltpu.VMEM((4, max(n_ch - RELAYED, 1), pair, WC), BF16),
                pltpu.VMEM((2, RELAYED, t_dev, WC), BF16),
                pltpu.VMEM((2, 3, RELAYED, pair, WC), BF16),
                pltpu.VMEM((n_ch, rows, WC), BF16),
                pltpu.VMEM((n_out, rows, WO), BF16),
                pltpu.VMEM((n_exp, cap, 2 * ffn), F32),
                pltpu.VMEM((n_exp, cap, ffn), BF16),
                pltpu.VMEM((n_exp, cap, WC), BF16),
                pltpu.VMEM((n_exp, cap, rows), BF16),
                pltpu.VMEM((n_exp, rows, cap), BF16),
                pltpu.VMEM((n_exp, rows, 128), F32),
                pltpu.VMEM((rows, WO), F32),
                pltpu.VMEM((groups, pair, t_dev), BF16),
                pltpu.VMEM((t_dev, rows), BF16),
                pltpu.VMEM((8, t_dev), F32),
                pltpu.VMEM((2, 8, t_dev), F32),
                pltpu.VMEM((groups, n_exp, 128), F32),
                pltpu.VMEM((groups, n_exp, 128), F32),
                pltpu.VMEM((DEPTH, WC, 2 * ffn), BF16),
                pltpu.VMEM((DEPTH2, ffn, WO), BF16),
                dma((n_ch,)), dma((2, n_ch)), dma((n_ch, 3)), dma((max(n_ch - RELAYED, 1), 4)), dma((n_ch, 2, 3)), dma((n_ch, groups)),
                dma((7,)), dma((groups,)), dma, dma((2,)),
                dma((n_out, 7)), dma((n_out, groups)), dma((2, DEPTH)), dma((DEPTH2,)),
                dma((3,)), dma((n_out,)),
            ],
            compiler_params=pltpu.CompilerParams(
                collective_id=0, has_side_effects=True, vmem_limit_bytes=67043328),
        )(tokens, expert_ids.T, gate_vals.T, w_gate, w_up, w_down)

    return jax.shard_map(device_step, mesh=mesh, in_specs=(row_spec, row_spec, row_spec, expert_spec, expert_spec, expert_spec), out_specs=row_spec, check_vma=False)
```

```python
import functools

import jax
import jax.numpy as jnp
from jax import lax
from jax.experimental import pallas as pl
from jax.experimental.pallas import tpu as pltpu
from jax.sharding import PartitionSpec as P

MESH = pl.DeviceIdType.MESH
F32, BF16 = jnp.float32, jnp.bfloat16
WC = 256
WO = 256
DEPTH = 8
DEPTH2 = 8
RELAYED = 4
AHEAD = 4
LATE = 4
UNROLL = 4
UNROLL2 = 8
FAR = 255.0


def flip(me, d):
    z, c = me // 2, me % 2
    hi, lo = z // 2, z % 2
    if d & 4:
        hi = 1 - hi
    if d & 2:
        lo = 1 - lo
    if d & 1:
        c = 1 - c
    return hi * 4 + lo * 2 + c


def dot(a, b):
    return jnp.dot(a, b, preferred_element_type=F32)


def dot_tn(a, b):
    return lax.dot_general(a, b, (((0,), (0,)), ((), ())), preferred_element_type=F32)


def dot_nt(a, b):
    return lax.dot_general(a, b, (((1,), (1,)), ((), ())), preferred_element_type=F32)


def iota(shape, dim):
    return lax.broadcasted_iota(jnp.int32, shape, dim)


def split3(g):
    hi = g.astype(BF16).astype(F32)
    rest = g - hi
    mid = rest.astype(BF16).astype(F32)
    return jnp.concatenate([hi, mid, rest - mid], axis=0).astype(BF16)


def kernel(tok_hbm, ids_hbm, gate_hbm, wg_hbm, wu_hbm, wd_hbm, out_hbm,
           tok, ids, gate, out, near, direct, raw, rly, xb, ret, acc, hid, xg, fan, fan_t, gb, ssum, pk, pt, pos, rpos, gsend, gtab,
           wgu, wd,
           raw_s, raw_r, near_s, far_s, rly_s, x_r, tab_s, tab_r, pos_s, pos_r, out_s, ret_r, w_s, wd_s, in_s, done_s):
    n_exp, cap, ffn = hid.shape
    t_dev = tok.shape[0]
    n_ch, rows, _ = xb.shape
    n_out = ret.shape[0]
    pair = rows // 8
    top_k = ids.shape[0]

    me = lax.axis_index("ep")
    core = me % 2
    side = me // 4
    lo = (me // 2) % 2
    is_mid = (lo + side) == 1
    relay_dev = (2 - side) * 2 + core
    far = 1 - side
    far_src = ((3 * far) * 2 + core, (1 + far) * 2 + core)
    my_rank = jnp.where(is_mid, 1, 0)
    peers = [flip(me, d) for d in range(8)]

    def remote(src, dst, s, r, dev):
        return pltpu.make_async_remote_copy(
            src_ref=src, dst_ref=dst, send_sem=s, recv_sem=r, device_id={"ep": dev}, device_id_type=MESH)

    def raw_copy(ch, j, dev):
        cols = pl.ds(pl.multiple_of(ch * WC, WC), WC)
        return remote(tok_hbm.at[:, cols], raw.at[j, ch], raw_s.at[ch], raw_r.at[j, ch], dev)

    def near_copy(ch, d):
        return remote(near.at[d - 1, ch], xb.at[ch, pl.ds(me * pair, pair)],
                      near_s.at[ch, d - 1], x_r.at[ch, me], peers[d])

    def far_copy(ch, d):
        return remote(direct.at[d - 4, ch - RELAYED], xb.at[ch, pl.ds(me * pair, pair)],
                      far_s.at[ch - RELAYED, d - 4], x_r.at[ch, me], peers[d])

    def rly_copy(ch, j, d):
        return remote(rly.at[j, d - 1, ch], xb.at[ch, pl.ds(far_src[j] * pair, pair)],
                      rly_s.at[ch, j, d - 1], x_r.at[ch, far_src[j]], peers[d])

    def x_wait(ch, src):
        remote(xb.at[ch, pl.ds(src * pair, pair)], xb.at[ch, pl.ds(src * pair, pair)],
               near_s.at[ch, 0], x_r.at[ch, src], peers[1]).wait_recv()

    def w_copies(i):
        ch, e, slot = i // n_exp, i % n_exp, i % DEPTH
        rws = pl.ds(pl.multiple_of(ch * WC, WC), WC)
        return (pltpu.make_async_copy(wg_hbm.at[e, rws], wgu.at[slot, :, pl.ds(0, ffn)], w_s.at[0, slot]),
                pltpu.make_async_copy(wu_hbm.at[e, rws], wgu.at[slot, :, pl.ds(ffn, ffn)], w_s.at[1, slot]))

    def wd_copy(i):
        ch, e, slot = i // n_exp, i % n_exp, i % DEPTH2
        cols = pl.ds(pl.multiple_of(ch * WO, WO), WO)
        return pltpu.make_async_copy(wd_hbm.at[e, :, cols], wd.at[slot], wd_s.at[slot])

    loads = [pltpu.make_async_copy(a, b, in_s.at[k]) for k, (a, b) in enumerate(
        ((ids_hbm, ids), (gate_hbm, gate), (tok_hbm, tok)))]
    for c in loads:
        c.start()
    barrier = pltpu.get_barrier_semaphore()
    for d in range(1, 8):
        pl.semaphore_signal(barrier, inc=1, device_id={"ep": peers[d]}, device_id_type=MESH)
    pl.semaphore_wait(barrier, 7)
    raw_copy(0, my_rank, relay_dev).start()
    for i in range(DEPTH):
        for c in w_copies(i):
            c.start()

    loads[0].wait()
    loads[1].wait()
    dev_iota = iota((8, t_dev), 0)
    chosen = jnp.zeros((8, t_dev), F32)
    for j in range(top_k):
        chosen = jnp.where(ids[j:j + 1, :] // n_exp == dev_iota, 1.0, chosen)
    tri = (iota((t_dev, t_dev), 0) <= iota((t_dev, t_dev), 1)).astype(F32).astype(BF16)
    rank = dot(chosen.astype(BF16), tri) - 1.0
    where = jnp.where(chosen > 0.0, rank, FAR)
    pos[...] = where
    pos_copy = remote(pos, rpos.at[my_rank], pos_s, pos_r.at[my_rank], relay_dev)
    slot_rows = iota((pair, t_dev), 0).astype(F32)
    for q in range(8):
        mat = (slot_rows == where[q:q + 1, :]).astype(F32).astype(BF16)
        pk[q] = mat
        dense = jnp.zeros((n_exp, t_dev), F32)
        for j in range(top_k):
            dense = jnp.where(ids[j:j + 1, :] == q * n_exp + dev_iota, gate[j:j + 1, :], dense)
        parts = dot_nt(split3(dense), mat)
        packed = (parts[n_exp:2 * n_exp] + parts[2 * n_exp:]) + parts[:n_exp]
        gsend[q, :, 0:pair] = packed

    def tab_copy(d):
        return remote(gsend.at[peers[d]], gtab.at[me], tab_s.at[d - 1], tab_r.at[me], peers[d])

    def tab_wait(d):
        remote(gsend.at[peers[d]], gtab.at[peers[d]], tab_s.at[d - 1], tab_r.at[peers[d]], peers[d]).wait_recv()

    pos_copy.start()
    for d in (7, 6, 5, 4, 3, 2, 1):
        tab_copy(d).start()
    gtab[me] = gsend[me]

    def near_send(ch):
        for d in (3, 2, 1):
            near_copy(ch, d).start()

    def far_send(ch, from_mid, from_end):
        @pl.when(is_mid)
        def _():
            for d in from_mid:
                far_copy(ch, d).start()

        @pl.when(jnp.logical_not(is_mid))
        def _():
            for d in from_end:
                far_copy(ch, d).start()

    def near_step(ch, _):
        cols = pl.ds(pl.multiple_of(ch * WC, WC), WC)
        block = tok[:, cols]

        @pl.when((ch > 0) & (ch < RELAYED))
        def _():
            raw_copy(ch, my_rank, relay_dev).start()

        @pl.when(ch >= RELAYED)
        def _():
            for d in (7, 6, 5, 4):
                direct[d - 4, ch - RELAYED] = dot(pk[peers[d]], block).astype(BF16)
            far_send(ch, (7, 6), (5, 4))

        for d in range(1, 4):
            near[d - 1, ch] = dot(pk[peers[d]], block).astype(BF16)
        xb[ch, pl.ds(me * pair, pair)] = dot(pk[me], block).astype(BF16)

        @pl.when(jnp.logical_not(is_mid) | (ch < AHEAD))
        def _():
            near_send(ch)
        return 0

    loads[2].wait()
    lax.fori_loop(0, n_ch, near_step, 0)
    for ch in range(RELAYED, n_ch):
        far_send(ch, (5, 4), ())

    for d in range(1, 8):
        tab_wait(d)
    gates = jnp.concatenate([gtab[p][:, :pair] for p in range(8)], axis=1)
    member = gates != 0.0
    tri_r = (iota((rows, rows), 0) <= iota((rows, rows), 1)).astype(F32).astype(BF16)
    count = dot(member.astype(F32).astype(BF16), tri_r) - 1.0
    place = jnp.where(member, count, FAR)
    cap_rows = iota((cap, rows), 0).astype(F32)
    for e in range(n_exp):
        fan[e] = (cap_rows == place[e:e + 1, :]).astype(F32).astype(BF16)

    def pos_wait(j):
        remote(pos, rpos.at[j], pos_s, pos_r.at[j], relay_dev).wait_recv()

    @pl.when(is_mid)
    def _():
        for j in range(2):
            pos_wait(j)

    def relay(ch):
        for j in range(2):
            raw_copy(ch, j, relay_dev).wait_recv()
            block = raw[j, ch]

            def packed(q):
                mat = (slot_rows == rpos[j, pl.ds(q, 1), :]).astype(F32).astype(BF16)
                return dot(mat, block).astype(BF16)

            for d in (3, 2, 1):
                rly[j, d - 1, ch] = packed(peers[d])
                rly_copy(ch, j, d).start()
            xb[ch, pl.ds(far_src[j] * pair, pair)] = packed(me)

        @pl.when(ch + AHEAD < n_ch)
        def _():
            near_send(ch + AHEAD)

    def group(ch, first, last):
        @pl.when(is_mid & (ch < RELAYED))
        def _():
            relay(ch)

        for d in range(1, 4):
            x_wait(ch, peers[d])

        straight = jnp.logical_not(is_mid) | (ch >= RELAYED)

        @pl.when(jnp.logical_not(straight))
        def _():
            for src in far_src:
                x_wait(ch, src + 1 - 2 * core)

        @pl.when(straight)
        def _():
            for d in range(4, 8):
                x_wait(ch, peers[d])

        block = xb[ch]
        for e in range(n_exp):
            xg[e] = dot(fan[e], block).astype(BF16)

        def experts(it, _):
            for u in range(UNROLL):
                for c in w_copies(ch * n_exp + it * UNROLL + u):
                    c.wait()
            for u in range(UNROLL):
                e = it * UNROLL + u
                slot = (ch * n_exp + e) % DEPTH
                both = dot(xg[e], wgu[slot])
                if not first:
                    both = acc[e] + both
                if last:
                    g = both[:, :ffn]
                    hid[e] = (g / (1.0 + jnp.exp(-g)) * both[:, ffn:]).astype(BF16)
                else:
                    acc[e] = both
                    i = ch * n_exp + it * UNROLL + u + DEPTH

                    @pl.when(i < n_ch * n_exp)
                    def _():
                        for c in w_copies(i):
                            c.start()
            return 0

        lax.fori_loop(0, n_exp // UNROLL, experts, 0)

    def middle_group(ch, _):
        @pl.when(ch == LATE)
        def _():
            for k in range(RELAYED, n_ch):
                far_send(k, (), (7, 6))

        group(ch, False, False)
        return 0

    def return_tables():
        lane = iota((8, rows), 1)
        base = iota((8, rows), 0) * pair
        blocks = ((lane >= base) & (lane < base + pair)).astype(F32).astype(BF16)
        spread = dot_tn(where.astype(BF16), blocks)
        lane_t = iota((t_dev, rows), 1)
        lane_s = lane_t
        for q in range(1, 8):
            lane_s = lane_s - jnp.where(lane_t >= q * pair, pair, 0)
        pt[...] = (spread == lane_s.astype(F32)).astype(F32).astype(BF16)

        place_b = place.astype(BF16)
        gate_parts = split3(gates)
        cap_lanes = iota((rows, cap), 1).astype(F32)
        for e in range(n_exp):
            pick = (iota((8, cap), 0) == e).astype(F32).astype(BF16)
            fan_t[e] = (dot_tn(place_b, pick) == cap_lanes).astype(F32).astype(BF16)
            pick3 = (lax.rem(iota((24, 128), 0), 8) == e).astype(F32).astype(BF16)
            gb[e] = dot_tn(gate_parts, pick3)

    group(0, True, False)
    for i in range(DEPTH2):
        wd_copy(i).start()
    return_tables()
    lax.fori_loop(1, n_ch - 1, middle_group, 0)
    group(n_ch - 1, False, True)

    def ret_copy(ch, d):
        return remote(xb.at[ch, pl.ds(peers[d] * pair, pair)], ret.at[ch, pl.ds(me * pair, pair)],
                      out_s.at[ch, d - 1], ret_r.at[ch, me], peers[d])

    def ret_wait(ch, d):
        src = peers[d]
        remote(xb.at[ch, pl.ds(src * pair, pair)], ret.at[ch, pl.ds(src * pair, pair)],
               out_s.at[ch, d - 1], ret_r.at[ch, src], src).wait_recv()

    def step_out(ch, _):
        def experts(it, _):
            first = ch * n_exp + it * UNROLL2
            for u in range(UNROLL2):
                wd_copy(first + u).wait()
            ys = [dot(hid[it * UNROLL2 + u], wd[(first + u) % DEPTH2]).astype(BF16) for u in range(UNROLL2)]
            add = None
            for u in range(UNROLL2):
                e = it * UNROLL2 + u
                z = dot(fan_t[e], ys[u])
                g = gb[e]
                part = jnp.concatenate([g * z[:, k * 128:(k + 1) * 128] for k in range(WO // 128)], axis=1)
                add = part if add is None else add + part

            @pl.when(it == 0)
            def _():
                ssum[...] = add

            @pl.when(it > 0)
            def _():
                ssum[...] += add

            for u in range(UNROLL2):
                @pl.when(first + u + DEPTH2 < n_out * n_exp)
                def _():
                    wd_copy(first + u + DEPTH2).start()
            return 0

        lax.fori_loop(0, n_exp // UNROLL2, experts, 0)
        xb[ch] = ssum[...].astype(BF16)
        ret[ch, pl.ds(me * pair, pair)] = ssum[pl.ds(me * pair, pair)].astype(BF16)
        for d in (7, 6, 5, 4, 3, 2, 1):
            ret_copy(ch, d).start()
        return 0

    def drain(ch, _):
        for d in range(1, 4):
            near_copy(ch, d).wait_send()

        @pl.when(ch < RELAYED)
        def _():
            raw_copy(ch, my_rank, relay_dev).wait_send()

        @pl.when(ch >= RELAYED)
        def _():
            for d in range(4, 8):
                far_copy(ch, d).wait_send()

        @pl.when(is_mid & (ch < RELAYED))
        def _():
            for j in range(2):
                for d in range(1, 4):
                    rly_copy(ch, j, d).wait_send()
        return 0

    lax.fori_loop(0, n_out, step_out, 0)
    lax.fori_loop(0, n_ch, drain, 0)
    pos_copy.wait_send()
    for d in range(1, 8):
        tab_copy(d).wait_send()

    def done_copy(ch):
        cols = pl.ds(pl.multiple_of(ch * WO, WO), WO)
        return pltpu.make_async_copy(out.at[ch], out_hbm.at[:, cols], done_s.at[ch])

    def step_end(ch, _):
        for d in range(1, 8):
            ret_wait(ch, d)
        cols = pl.ds(pl.multiple_of(ch * WO, WO), WO)
        out[ch] = (tok[:, cols].astype(F32) + dot(pt[...], ret[ch])).astype(BF16)
        done_copy(ch).start()
        return 0

    lax.fori_loop(0, n_out, step_end, 0)

    def drain_out(ch, _):
        for d in range(1, 8):
            ret_copy(ch, d).wait_send()
        done_copy(ch).wait()
        return 0

    lax.fori_loop(0, n_out, drain_out, 0)


def solution(mesh):
    groups = mesh.shape['ep']
    row_spec = P(('dp', 'ep'))
    expert_spec = P('ep')

    def device_step(tokens, expert_ids, gate_vals, w_gate, w_up, w_down):
        t_dev, top_k = expert_ids.shape
        d_model = tokens.shape[1]
        n_exp, _, ffn = w_gate.shape
        pair = t_dev * (top_k // 2) // groups
        cap = t_dev * top_k // n_exp
        rows = groups * pair
        n_ch, n_out = d_model // WC, d_model // WO
        hbm = pl.BlockSpec(memory_space=pl.ANY)
        dma = pltpu.SemaphoreType.DMA
        return pl.pallas_call(
            kernel,
            out_shape=jax.ShapeDtypeStruct((t_dev, d_model), BF16),
            in_specs=[hbm] * 6,
            out_specs=hbm,
            scratch_shapes=[
                pltpu.VMEM((t_dev, d_model), BF16),
                pltpu.VMEM((top_k, t_dev), jnp.int32),
                pltpu.VMEM((top_k, t_dev), F32),
                pltpu.VMEM((n_out, t_dev, WO), BF16),
                pltpu.VMEM((3, n_ch, pair, WC), BF16),
                pltpu.VMEM((4, max(n_ch - RELAYED, 1), pair, WC), BF16),
                pltpu.VMEM((2, RELAYED, t_dev, WC), BF16),
                pltpu.VMEM((2, 3, RELAYED, pair, WC), BF16),
                pltpu.VMEM((n_ch, rows, WC), BF16),
                pltpu.VMEM((n_out, rows, WO), BF16),
                pltpu.VMEM((n_exp, cap, 2 * ffn), F32),
                pltpu.VMEM((n_exp, cap, ffn), BF16),
                pltpu.VMEM((n_exp, cap, WC), BF16),
                pltpu.VMEM((n_exp, cap, rows), BF16),
                pltpu.VMEM((n_exp, rows, cap), BF16),
                pltpu.VMEM((n_exp, rows, 128), F32),
                pltpu.VMEM((rows, WO), F32),
                pltpu.VMEM((groups, pair, t_dev), BF16),
                pltpu.VMEM((t_dev, rows), BF16),
                pltpu.VMEM((8, t_dev), F32),
                pltpu.VMEM((2, 8, t_dev), F32),
                pltpu.VMEM((groups, n_exp, 128), F32),
                pltpu.VMEM((groups, n_exp, 128), F32),
                pltpu.VMEM((DEPTH, WC, 2 * ffn), BF16),
                pltpu.VMEM((DEPTH2, ffn, WO), BF16),
                dma((n_ch,)), dma((2, n_ch)), dma((n_ch, 3)), dma((max(n_ch - RELAYED, 1), 4)), dma((n_ch, 2, 3)), dma((n_ch, groups)),
                dma((7,)), dma((groups,)), dma, dma((2,)),
                dma((n_out, 7)), dma((n_out, groups)), dma((2, DEPTH)), dma((DEPTH2,)),
                dma((3,)), dma((n_out,)),
            ],
            compiler_params=pltpu.CompilerParams(
                collective_id=0, has_side_effects=True, vmem_limit_bytes=67043328),
        )(tokens, expert_ids.T, gate_vals.T, w_gate, w_up, w_down)

    return jax.shard_map(device_step, mesh=mesh, in_specs=(row_spec, row_spec, row_spec, expert_spec, expert_spec, expert_spec), out_specs=row_spec, check_vma=False)
```
